512 devices in a mesh: parts: 2 (over y), tm: 32 (over z, core), band: 8 (over x).
Axes of the slice: x: 8, y: 2, z: 16, core: 2. Of those that a mesh axis runs over, the one named last changes fastest.
The devices are a block of a 8x8x16 slice.
Arguments:
- baseband: bfloat16 [32, 4, 3145728], P('band', None, ('parts', 'tm')), parts along dimension 2, may hold values from -6 to 6
- intersection: int32 [64, 32], P(('parts', 'tm'), 'band'), parts along dimension 0, may hold values from 8192 to 16384
- chirp_phase: float32 [4, 65536], replicated, may hold values from -1 to 45875
- chirp_index: int32 [64], P(('parts', 'band')), parts along dimension 0, may hold values from 0 to 3
- phase_bins: int32 [49152], P(('parts', 'tm')), parts along dimension 0, may hold values from 0 to 511
Outputs:
- profiles: float32 [128, 32, 4, 512], P(('parts', 'tm'), 'band'), parts along dimension 0
The draws below stay inside these ranges and needn't reach their ends.
There are 2 independent parts, one for each index of `parts`. The reference program is written for one: setup_inputs(seed, part) draws one part's arguments, and reference() takes and returns one part's arrays. A program takes and returns all parts, laid end to end along the dimension named above; an argument that names none is the same for every part. Nothing has to cross between parts.
All inputs are finite; a program needn't handle non-finite values.
Results may differ from the reference program's by a relative error of at most 0.0049.
Values may be sent and summed in bfloat16 or wider, within the bound.
A program may use at most 64 MiB of HBM per device.

```python
import math
import jax
import jax.numpy as jnp
from jax import lax

CHANNELS = 32
SEGS = 32
SIDE = 256
SEGLEN = 65536
OVL = 16384
STEP = 49152
FINE = 64
FINELEN = 1024
OUTLEN = 24576
SAMPLES = 1572864
BINS = 512
NDM = 4


def draw_chirp_phase(key, part):
    key_span, key_curve, key_jitter = jax.random.split(jax.random.fold_in(key, 11), 3)
    spans = jax.random.uniform(key_span, (NDM, 1), minval=0.4 * OVL, maxval=0.8 * OVL)
    curves = jax.random.uniform(key_curve, (NDM, 1), minval=-0.2, maxval=0.2)
    frequency = jnp.arange(SEGLEN, dtype=jnp.int32)
    offset = ((frequency + SEGLEN // 2) % SEGLEN).astype(jnp.float32) / SEGLEN
    jitter = jax.random.uniform(key_jitter, (NDM, SEGLEN), minval=-1.0, maxval=1.0)
    return (math.pi * spans * offset * offset / (1.0 + curves * (offset - 0.5)) + jitter).astype(jnp.float32)


def draw_phase_bins(key, part):
    key_rate, key_anchor = jax.random.split(jax.random.fold_in(key, 23))
    advance = jax.random.randint(key_rate, (), 2048, 4097)
    anchor = jax.random.randint(key_anchor, (), 0, BINS)
    sample_index = jnp.arange(OUTLEN, dtype=jnp.int32)
    return ((anchor + sample_index * advance // 4096) % BINS).astype(jnp.int32)


def with_ends(drawn, key, low, largest):
    spot = [jax.random.randint(jax.random.fold_in(key, axis), (), 0, length) for axis, length in enumerate(drawn.shape)]
    widest = drawn.shape.index(max(drawn.shape))
    beside = spot[:widest] + [(spot[widest] + 1) % drawn.shape[widest]] + spot[widest + 1:]
    return drawn.at[tuple(spot)].set(low).at[tuple(beside)].set(largest)


def shard_levels(key, extent, cuts, least, top_value):
    level, own = 1.0, jax.random.fold_in(key, 6)
    for position, parts in cuts:
        draws = jnp.exp(jax.random.uniform(jax.random.fold_in(own, position), (parts,), jnp.float32, least / len(cuts), top_value / len(cuts)))
        level = level * jnp.repeat(draws, extent[position] // parts).reshape([-1 if axis == position else 1 for axis in range(len(extent))])
    return level


def centred(key, shape, scale, reach, cuts=(), kind=jnp.bfloat16):
    loudness = shard_levels(key, shape, cuts, -0.22, 0.18) if cuts else 1.0
    values = jax.random.normal(key, shape, jnp.float32) * scale * loudness
    return jnp.minimum(jnp.maximum(values, -reach), reach).astype(kind)


def setup_inputs(seed: int = 0, part: int = 0) -> dict:
    arg_keys = jax.random.split(jax.random.key(seed), 6)
    part_keys = jax.random.split(jax.random.fold_in(arg_keys[5], part), 6)
    return {
        "baseband": centred(part_keys[0], (CHANNELS, 4, SAMPLES), 1.0, 6.0, ((0, 8), (2, 32))),
        "intersection": with_ends(jax.random.randint(part_keys[1], (SEGS, CHANNELS), OVL // 2, OVL + 1), jax.random.fold_in(part_keys[1], 1), OVL // 2, OVL).astype(jnp.int32),
        "chirp_phase": draw_chirp_phase(jax.random.fold_in(arg_keys[5], 71), part),
        "chirp_index": with_ends(jax.random.randint(part_keys[3], (CHANNELS,), 0, NDM), jax.random.fold_in(part_keys[3], 1), 0, NDM - 1).astype(jnp.int32),
        "phase_bins": draw_phase_bins(jax.random.fold_in(jax.random.fold_in(arg_keys[5], part), 71), part),
    }


def reference(baseband, intersection, chirp_phase, chirp_index, phase_bins):
    onehot = (phase_bins[:, None] == jnp.arange(BINS, dtype=jnp.int32)[None, :]).astype(jnp.bfloat16)
    phases = chirp_phase[chirp_index]
    positions = jnp.arange(OVL, dtype=jnp.int32)

    def one_channel(inputs):
        samples, counts, phase_row = inputs
        blocks = samples.astype(jnp.float32).reshape(4, SEGS, STEP)
        tail_rows = jnp.concatenate([jnp.zeros((4, 1, OVL), jnp.float32), blocks[:, :-1, STEP - OVL:]], axis=1)
        usable = positions[None, :] >= (OVL - counts)[:, None]
        tail_rows = jnp.where(usable[None], tail_rows, jnp.zeros_like(tail_rows))
        window = jnp.concatenate([tail_rows, blocks], axis=2)
        fields = jnp.stack([window[0] + 1j * window[1], window[2] + 1j * window[3]])
        spectrum = jnp.fft.fft(fields, axis=-1) / SIDE
        spectrum = spectrum * jnp.exp(-1j * phase_row)
        shifted = jnp.roll(spectrum, SEGLEN // 2, axis=-1).reshape(2, SEGS, FINE, FINELEN)
        fine_waves = jnp.fft.ifft(shifted, axis=-1) * math.sqrt(FINELEN)
        fine_waves = fine_waves[..., OVL // FINE:]
        first_pol = fine_waves[0]
        second_pol = fine_waves[1]
        first_power = jnp.real(first_pol) ** 2 + jnp.imag(first_pol) ** 2
        second_power = jnp.real(second_pol) ** 2 + jnp.imag(second_pol) ** 2
        cross_term = first_pol * jnp.conj(second_pol)
        stokes = jnp.stack([first_power + second_power, first_power - second_power, 2.0 * jnp.real(cross_term), 2.0 * jnp.imag(cross_term)])
        stokes = stokes.astype(jnp.bfloat16).transpose(2, 0, 1, 3).reshape(FINE * 4, OUTLEN)
        folded = jnp.dot(stokes, onehot, preferred_element_type=jnp.float32)
        return folded.reshape(FINE, 4, BINS) * (BINS / OUTLEN)
    result = lax.map(one_channel, (baseband, intersection.T, phases))
    return result.transpose(1, 0, 2, 3)
```

```python
import functools
import math

import jax
import jax.numpy as jnp
import numpy as np
from jax import lax
from jax.experimental import pallas as pl
from jax.experimental.pallas import tpu as pltpu
from jax.sharding import PartitionSpec as P

SIDE = 256
FINE = 64
BINS = 512
SUB = SIDE // FINE
LANES = 128
MESH = pl.DeviceIdType.MESH


def fine_order(owners):
    per = FINE // owners
    places = owners // 2
    return np.array(
        [per * (2 * z + p) + i for p in range(2) for i in range(per) for z in range(places)]
    )


def half(values):
    return np.asarray(values, np.float32).astype(jnp.bfloat16)


def unit_gain(table):
    found, seen = np.empty_like(table), {}
    scales = 1.0 + np.arange(0, 2001) * 1e-6 * np.where(np.arange(2001) % 2, 1, -1)
    for k, row in enumerate(table):
        key = math.gcd(k, len(table))
        if key not in seen:
            tried = scales[:, None] * row[None, :]
            tried = half(tried.real).astype(np.float64) + 1j * half(tried.imag).astype(np.float64)
            gain = (tried * row.conj()).real.mean(axis=1)
            seen[key] = scales[np.argmin(np.abs(gain - 1.0))]
        scaled = seen[key] * row
        found[k] = half(scaled.real).astype(np.float64) + 1j * half(scaled.imag).astype(np.float64)
    return found


@functools.lru_cache(maxsize=None)
def tables(owners):
    idx = np.arange(SIDE)
    base = 2.0 * np.pi * (np.outer(idx, idx) % SIDE) / SIDE
    unit = unit_gain(np.exp(1j * base))
    cos, sin = unit.real, unit.imag
    first = np.block([[cos, sin], [-sin, cos]])
    order = (fine_order(owners) + FINE // 2) % FINE
    rows = np.concatenate([SUB * order + r for r in range(SUB)])
    second = np.block([[cos[rows], sin[rows]], [-sin[rows], cos[rows]]]) / SIDE
    inverse = np.block([[cos.T, sin.T], [-sin.T, cos.T]]) / math.sqrt(SIDE * SUB)
    turn = 2.0 * np.pi * np.outer(idx, idx) / (SIDE * SIDE)
    turns = np.stack([np.cos(turn), np.sin(turn)])
    inner = 2.0 * np.pi * np.outer(np.arange(SUB), idx) / (SIDE * SUB)
    inners = np.stack([np.cos(inner), np.sin(inner)])
    return (
        half(first),
        half(second),
        half(inverse),
        turns.astype(np.float32),
        inners.astype(np.float32),
    )


def sincos(phase):
    turns = jnp.floor(phase * np.float32(2.0 / np.pi) + 0.5)
    step = np.pi / 2.0
    high = np.float32(np.round(step * 2**7) / 2**7)
    mid = np.float32(np.round((step - float(high)) * 2**17) / 2**17)
    low = np.float32(step - float(high) - float(mid))
    rest = ((phase - turns * high) - turns * mid) - turns * low
    quarter = turns.astype(jnp.int32) & 3
    sq = rest * rest
    sin = rest + rest * sq * (
        np.float32(-1.6666654611e-1)
        + sq * (np.float32(8.3321608736e-3) + sq * np.float32(-1.9515295891e-4))
    )
    cos = (
        np.float32(1.0)
        - np.float32(0.5) * sq
        + sq
        * sq
        * (
            np.float32(4.166664568298827e-2)
            + sq * (np.float32(-1.388731625493765e-3) + sq * np.float32(2.443315711809948e-5))
        )
    )
    odd = (quarter & 1) == 1
    sin_out = jnp.where(odd, cos, sin)
    cos_out = jnp.where(odd, sin, cos)
    sin_out = jnp.where(quarter >= 2, -sin_out, sin_out)
    cos_out = jnp.where((quarter == 1) | (quarter == 2), -cos_out, cos_out)
    return sin_out, cos_out


def prepare_kernel(owners, index_ref, phase_ref, bins_ref, waves_ref, onehot_ref):
    c = pl.program_id(0)
    row = index_ref[c]
    per = FINE // owners
    places = owners // 2
    eights = SIDE * 8 // FINE
    stride = 2 * per * eights
    for r in range(SUB):
        for p in range(2):
            for i in range(per):
                for g in range(places // 8):
                    fine = (per * (2 * 8 * g + p) + i + FINE // 2) % FINE
                    start = eights * fine + 8 * r
                    to = r * FINE + (p * per + i) * places + 8 * g
                    for h in range(2):
                        phase = phase_ref[pl.ds(start + 4 * h + row, 8, stride=stride), :]
                        sin, cos = sincos(phase)
                        waves_ref[0, 0, to : to + 8, h * LANES : (h + 1) * LANES] = cos
                        waves_ref[0, 1, to : to + 8, h * LANES : (h + 1) * LANES] = sin
    mine = bins_ref[pl.ds(c, 1), :]
    numbers = lax.broadcasted_iota(jnp.int32, (BINS, SIDE), 0)
    onehot_ref[:, :] = (numbers == mine).astype(jnp.float32).astype(jnp.bfloat16)


def transform_kernel(
    owners,
    counts_ref,
    new_ref,
    old_ref,
    first_ref,
    second_ref,
    inverse_ref,
    turns_ref,
    inners_ref,
    waves_ref,
    onehot_ref,
    out_ref,
    flat,
    window,
    section,
    turned,
    spectrum,
    mixed,
    waves,
    stokes,
):
    c = pl.program_id(0)
    margin_rows = old_ref.shape[1]
    rows = lax.broadcasted_iota(jnp.int32, (margin_rows, LANES), 0)
    lanes = lax.broadcasted_iota(jnp.int32, (margin_rows, LANES), 1)
    position = SIDE * (rows // 8) + LANES * ((rows // 4) % 2) + lanes
    usable = position >= (SIDE * SIDE // 4 - counts_ref[c])
    flat[:margin_rows, :] = jnp.where(usable, old_ref[0].astype(jnp.float32), 0.0)
    flat[margin_rows:, :] = new_ref[0].astype(jnp.float32)
    for p in range(2):
        for part in range(2):
            for h in range(2):
                piece = flat[pl.ds(4 * h + 2 * p + part, SIDE, stride=8), :]
                window[
                    part * SIDE : (part + 1) * SIDE,
                    p * SIDE + h * LANES : p * SIDE + (h + 1) * LANES,
                ] = piece.astype(jnp.bfloat16)
    section[...] = jnp.dot(first_ref[...], window[...], preferred_element_type=jnp.float32)
    for i in range(0, SIDE, 16):
        for h in range(0, SIDE, LANES):
            cos = turns_ref[0, i : i + 16, h : h + LANES]
            sin = turns_ref[1, i : i + 16, h : h + LANES]
            for p in range(2):
                at = slice(p * SIDE + h, p * SIDE + h + LANES)
                re = section[i : i + 16, at]
                im = section[SIDE + i : SIDE + i + 16, at]
                to = slice(p * SIDE + i, p * SIDE + i + 16)
                turned[to, h : h + LANES] = (re * cos + im * sin).astype(jnp.bfloat16)
                turned[to, SIDE + h : SIDE + h + LANES] = (im * cos - re * sin).astype(
                    jnp.bfloat16
                )
    spectrum[...] = lax.dot_general(
        second_ref[...],
        turned[...],
        (((1,), (1,)), ((), ())),
        preferred_element_type=jnp.float32,
    )
    for h in range(0, SIDE, LANES):
        inner = [
            (inners_ref[0, o : o + 1, h : h + LANES], inners_ref[1, o : o + 1, h : h + LANES])
            for o in range(SUB)
        ]
        for i in range(0, FINE, 16):
            for p in range(2):
                at = slice(p * SIDE + h, p * SIDE + h + LANES)
                d_re, d_im = [], []
                for r in range(SUB):
                    src = r * FINE + i
                    re = spectrum[src : src + 16, at]
                    im = spectrum[SIDE + src : SIDE + src + 16, at]
                    cos = waves_ref[0, 0, src : src + 16, h : h + LANES]
                    sin = waves_ref[0, 1, src : src + 16, h : h + LANES]
                    d_re.append(re * cos + im * sin)
                    d_im.append(im * cos - re * sin)
                even_re, even_im = d_re[0] + d_re[2], d_im[0] + d_im[2]
                less_re, less_im = d_re[0] - d_re[2], d_im[0] - d_im[2]
                odd_re, odd_im = d_re[1] + d_re[3], d_im[1] + d_im[3]
                gap_re, gap_im = d_re[1] - d_re[3], d_im[1] - d_im[3]
                totals = [
                    (even_re + odd_re, even_im + odd_im),
                    (less_re - gap_im, less_im + gap_re),
                    (even_re - odd_re, even_im - odd_im),
                    (less_re + gap_im, less_im - gap_re),
                ]
                for o in range(SUB):
                    re, im = totals[o]
                    if o:
                        cos, sin = inner[o]
                        re, im = re * cos - im * sin, re * sin + im * cos
                    to = slice(o * 2 * FINE + p * FINE + i, o * 2 * FINE + p * FINE + i + 16)
                    mixed[to, h : h + LANES] = re.astype(jnp.bfloat16)
                    mixed[to, SIDE + h : SIDE + h + LANES] = im.astype(jnp.bfloat16)
    waves[...] = jnp.dot(mixed[...], inverse_ref[...], preferred_element_type=jnp.float32)
    for o in range(SUB):
        for i in range(0, FINE, 16):
            for h in range(0, SIDE, LANES):
                src = o * 2 * FINE + i
                x_re = waves[src : src + 16, h : h + LANES]
                x_im = waves[src : src + 16, SIDE + h : SIDE + h + LANES]
                y_re = waves[src + FINE : src + FINE + 16, h : h + LANES]
                y_im = waves[src + FINE : src + FINE + 16, SIDE + h : SIDE + h + LANES]
                x_power = x_re * x_re + x_im * x_im
                y_power = y_re * y_re + y_im * y_im
                values = (
                    x_power + y_power,
                    x_power - y_power,
                    2.0 * (x_re * y_re + x_im * y_im),
                    2.0 * (x_im * y_re - x_re * y_im),
                )
                for v in range(4):
                    stokes[
                        v * FINE + i : v * FINE + i + 16, o * SIDE + h : o * SIDE + h + LANES
                    ] = values[v].astype(jnp.bfloat16)
    folded = lax.dot_general(
        stokes[...],
        onehot_ref[...],
        (((1,), (1,)), ((), ())),
        preferred_element_type=jnp.float32,
    )
    per = FINE // owners
    places = owners // 2
    for v in range(4):
        for p in range(2):
            for i in range(per):
                src = v * FINE + (p * per + i) * places
                for q in range(BINS // LANES):
                    out_ref[0, p, q, pl.ds(4 * i + v, places, stride=4 * per), :] = folded[
                        src : src + places, q * LANES : (q + 1) * LANES
                    ]


def reduce_kernel(
    scale,
    partial_ref,
    out_ref,
    own,
    paired,
    send_right,
    send_left,
    from_left,
    from_right,
    pair_send,
    pair_recv,
    right_send,
    right_recv,
    left_send,
    left_recv,
):
    channels = partial_ref.shape[0]
    owners = lax.axis_size("tm")
    places = owners // 2
    steps = places // 2
    tile = own.shape[2] // places
    me = lax.axis_index("tm")
    place = me // 2
    core = me % 2
    partner = {"tm": place * 2 + 1 - core}
    right = {"tm": ((place + 1) % places) * 2 + core}
    left = {"tm": ((place + places - 1) % places) * 2 + core}

    barrier = pltpu.get_barrier_semaphore()
    for device in (partner, right, left):
        pl.semaphore_signal(barrier, inc=1, device_id=device, device_id_type=MESH)
    pl.semaphore_wait(barrier, 3)

    def pair_copy(c):
        return pltpu.make_async_remote_copy(
            src_ref=partial_ref.at[c, 1 - core],
            dst_ref=paired.at[c],
            send_sem=pair_send.at[c],
            recv_sem=pair_recv.at[c],
            device_id=partner,
            device_id_type=MESH,
        )

    def right_copy(s, c):
        return pltpu.make_async_remote_copy(
            src_ref=send_right.at[s, c],
            dst_ref=from_left.at[s, c],
            send_sem=right_send.at[s, c],
            recv_sem=right_recv.at[s, c],
            device_id=right,
            device_id_type=MESH,
        )

    def left_copy(s, c):
        return pltpu.make_async_remote_copy(
            src_ref=send_left.at[s, c],
            dst_ref=from_right.at[s, c],
            send_sem=left_send.at[s, c],
            recv_sem=left_recv.at[s, c],
            device_id=left,
            device_id_type=MESH,
        )

    def block(c, where):
        return own[c, :, pl.ds(pl.multiple_of(where * tile, tile), tile), :]

    for c in range(channels):
        pair_copy(c).start()
    for c in range(channels):
        pair_copy(c).wait()
        own[c] = partial_ref[c, core] + paired[c]
        send_right[0, c] = block(c, (place + steps) % places)
        right_copy(0, c).start()
        send_left[0, c] = block(c, (place + places - steps + 1) % places)
        left_copy(0, c).start()

    def step(s, carry):
        for c in range(channels):
            right_copy(s - 1, c).wait()
            send_right[s, c] = from_left[s - 1, c] + block(c, (place + steps - s) % places)
            right_copy(s, c).start()
            left_copy(s - 1, c).wait()
            send_left[s, c] = from_right[s - 1, c] + block(
                c, (place + places - steps + 1 + s) % places
            )
            left_copy(s, c).start()
        return carry

    lax.fori_loop(1, steps - 1, step, 0)
    last = steps - 1
    for c in range(channels):
        right_copy(last - 1, c).wait()
        send_right[last, c] = from_left[last - 1, c] + block(c, (place + 1) % places)
        right_copy(last, c).start()
    for c in range(channels):
        left_copy(last - 1, c).wait()
        right_copy(last, c).wait()
        total = (from_left[last, c] + from_right[last - 1, c] + block(c, place)) * scale
        per = tile // 4
        for i in range(per):
            for q in range(total.shape[0]):
                out_ref[i, c, :, q * LANES : (q + 1) * LANES] = total[q, 4 * i : 4 * i + 4, :]


def local(baseband, intersection, chirp_phase, chirp_index, phase_bins):
    channels = baseband.shape[0]
    samples = baseband.shape[2]
    owners = lax.axis_size("tm")
    margin = SIDE * SIDE // 4
    per = FINE // owners
    first, second, inverse, turns, inners = [jnp.asarray(a) for a in tables(owners)]

    def as_rows(block):
        tiles = block.shape[2] // LANES
        return (
            block.reshape(channels, 4, tiles, LANES)
            .transpose(0, 2, 1, 3)
            .reshape(channels, 4 * tiles, LANES)
        )

    outgoing = baseband[:, :, samples - margin :]
    route = [(i - 1, i) for i in range(1, owners)]
    arrived = lax.ppermute(outgoing, "tm", route)
    phases = (
        chirp_phase.reshape(4, SIDE * 2, LANES).transpose(1, 0, 2).reshape(SIDE * 8, LANES)
    )
    bins = jnp.pad(
        phase_bins.reshape(-1, SUB).T, ((0, 0), (SIDE // 4, 0)), constant_values=-1
    )
    vmem = pltpu.MemorySpace.VMEM
    smem = pltpu.MemorySpace.SMEM
    whole = lambda shape: pl.BlockSpec(shape, lambda c: (0,) * len(shape))
    chirps, onehot = pl.pallas_call(
        functools.partial(prepare_kernel, owners),
        grid=(channels,),
        out_shape=(
            jax.ShapeDtypeStruct((channels, 2, SIDE, SIDE), jnp.float32),
            jax.ShapeDtypeStruct((BINS, SUB * SIDE), jnp.bfloat16),
        ),
        in_specs=[
            pl.BlockSpec(memory_space=smem),
            whole((SIDE * 8, LANES)),
            whole((SUB, SIDE)),
        ],
        out_specs=(
            pl.BlockSpec((1, 2, SIDE, SIDE), lambda c: (c, 0, 0, 0)),
            pl.BlockSpec((BINS, SIDE), lambda c: (0, c)),
        ),
        cost_estimate=pl.CostEstimate(
            flops=50_000_000, bytes_accessed=4_000_000, transcendentals=0
        ),
        name="prepare",
    )(chirp_index, phases, bins)
    partial = pl.pallas_call(
        functools.partial(transform_kernel, owners),
        grid=(channels,),
        out_shape=jax.ShapeDtypeStruct(
            (channels, 2, BINS // LANES, 4 * FINE // 2, LANES), jnp.float32
        ),
        in_specs=[
            pl.BlockSpec(memory_space=smem),
            pl.BlockSpec((1, samples * 4 // LANES, LANES), lambda c: (c, 0, 0)),
            pl.BlockSpec((1, margin * 4 // LANES, LANES), lambda c: (c, 0, 0)),
            whole((2 * SIDE, 2 * SIDE)),
            whole((2 * SIDE, 2 * SIDE)),
            whole((2 * SIDE, 2 * SIDE)),
            whole((2, SIDE, SIDE)),
            whole((2, SUB, SIDE)),
            pl.BlockSpec((1, 2, SIDE, SIDE), lambda c: (c, 0, 0, 0)),
            whole((BINS, SUB * SIDE)),
        ],
        out_specs=pl.BlockSpec(
            (1, 2, BINS // LANES, 4 * FINE // 2, LANES), lambda c: (c, 0, 0, 0, 0)
        ),
        scratch_shapes=[
            pltpu.VMEM((SIDE * 8, LANES), jnp.float32),
            pltpu.VMEM((2 * SIDE, 2 * SIDE), jnp.bfloat16),
            pltpu.VMEM((2 * SIDE, 2 * SIDE), jnp.float32),
            pltpu.VMEM((2 * SIDE, 2 * SIDE), jnp.bfloat16),
            pltpu.VMEM((2 * SIDE, 2 * SIDE), jnp.float32),
            pltpu.VMEM((2 * SUB * FINE, 2 * SIDE), jnp.bfloat16),
            pltpu.VMEM((2 * SUB * FINE, 2 * SIDE), jnp.float32),
            pltpu.VMEM((4 * FINE, SUB * SIDE), jnp.bfloat16),
        ],
        cost_estimate=pl.CostEstimate(
            flops=4_000_000_000, bytes_accessed=10_000_000, transcendentals=0
        ),
        name="transform",
    )(
        intersection.reshape(channels),
        as_rows(baseband),
        as_rows(arrived),
        first,
        second,
        inverse,
        turns,
        inners,
        chirps,
        onehot,
    )
    places = owners // 2
    steps = places // 2
    quarters = BINS // LANES
    chunk = (quarters, 4 * per, LANES)
    scale = np.float32(BINS / (phase_bins.shape[0] * owners))
    return pl.pallas_call(
        functools.partial(reduce_kernel, scale),
        out_shape=jax.ShapeDtypeStruct((per, channels, 4, BINS), jnp.float32),
        in_specs=[pl.BlockSpec(memory_space=vmem)],
        out_specs=pl.BlockSpec(memory_space=vmem),
        scratch_shapes=[
            pltpu.VMEM((channels, quarters, 4 * per * places, LANES), jnp.float32),
            pltpu.VMEM((channels, quarters, 4 * per * places, LANES), jnp.float32),
            pltpu.VMEM((steps, channels) + chunk, jnp.float32),
            pltpu.VMEM((steps - 1, channels) + chunk, jnp.float32),
            pltpu.VMEM((steps, channels) + chunk, jnp.float32),
            pltpu.VMEM((steps - 1, channels) + chunk, jnp.float32),
            pltpu.SemaphoreType.DMA((channels,)),
            pltpu.SemaphoreType.DMA((channels,)),
            pltpu.SemaphoreType.DMA((steps, channels)),
            pltpu.SemaphoreType.DMA((steps, channels)),
            pltpu.SemaphoreType.DMA((steps - 1, channels)),
            pltpu.SemaphoreType.DMA((steps - 1, channels)),
        ],
        compiler_params=pltpu.CompilerParams(collective_id=0, has_side_effects=True),
        name="reduce",
    )(partial)


def solution(mesh):
    return jax.shard_map(
        local,
        mesh=mesh,
        in_specs=(
            P("band", None, ("parts", "tm")),
            P(("parts", "tm"), "band"),
            P(),
            P(("parts", "band")),
            P(("parts", "tm")),
        ),
        out_specs=P(("parts", "tm"), "band", None, None),
        check_vma=False,
    )
```
